32 devices in a mesh: bank: 2 (over y), zero: 16 (over z, x, core).
Axes of the slice: x: 2, y: 2, z: 4, core: 2. Of those that a mesh axis runs over, the one named last changes fastest.
Arguments:
- train_down: float32 [16, 6400, 4096], P('bank', None, 'zero'), may hold values from -0.109375 to 0.109375
- other_down: bfloat16 [16, 6400, 4096], P('bank', None, 'zero'), may hold values from -0.0390625 to 0.0390625
- router_weight: float32 [4096, 16], P('zero', 'bank'), may hold values from -0.09375 to 0.09375
- router_gain: float32 [4096], P('zero'), may hold values from 0.25 to 1.75
Outputs:
- ready_down: bfloat16 [16, 6400, 4096], P('bank', 'zero')
- scale_down: float32 [16, 6400], P('bank', 'zero')
- serve_router: bfloat16 [4096, 16], replicated
The draws below stay inside these ranges and needn't reach their ends.
All inputs are finite; a program needn't handle non-finite values. Where the reference program divides by a largest or mean magnitude, that divisor is 1e-20 or more.
Results may differ from the reference program's by a relative error of at most 0.001.
Values may be sent and summed in bfloat16 or wider, within the bound.
A program may use at most 256 MiB of HBM per device.

```python
import jax
import jax.numpy as jnp

EXPERTS = 16
D_MODEL = 4096
D_EXPERT = 6400


def raised(values, key, source, target, shards_of, factor):
    owner, partner = [(jnp.arange(values.shape[dim]) // (values.shape[dim] // shards_of)).reshape([-1 if axis == dim else 1 for axis in range(values.ndim)]) for dim in (source, target)]
    chosen = jax.random.permutation(key, shards_of)[partner]
    strong = (owner == chosen) | (owner == (partner + shards_of // 2) % shards_of)
    return jnp.where(strong, factor * values, values)


def level_of(key, dims, cuts, least, high):
    loudness = 1.0
    for dim, blocks in cuts:
        draws = jax.random.uniform(jax.random.fold_in(jax.random.fold_in(key, 6), dim), (blocks,), jnp.float32, least / len(cuts), high / len(cuts))
        loudness = loudness * jnp.repeat(jnp.exp(draws), dims[dim] // blocks).reshape((-1,) + (1,) * (len(dims) - 1 - dim))
    return loudness


def noise(rng, dims, deviation, reach, pieces=(), held_as=jnp.bfloat16):
    result = jax.random.normal(rng, dims, jnp.float32) * deviation
    if len(pieces) > 0:
        result = level_of(rng, dims, pieces, -0.22, 0.18) * result
    return jnp.clip(result, min=-reach, max=reach).astype(held_as)


def bell_draw_with(key, extent, scale, limit, pieces, heavy, dtype=jnp.bfloat16):
    array = scale * jax.random.normal(key, extent, jnp.float32)
    if pieces:
        array = array * level_of(key, extent, pieces, -0.22, 0.18)
    return jnp.clip(raised(array, jax.random.fold_in(key, 3), *heavy), -limit, limit).astype(dtype)


def setup_inputs(seed: int = 0) -> dict:
    streams_of = jax.random.split(jax.random.key(seed), 5)
    train_down = bell_draw_with(streams_of[0], (EXPERTS, D_EXPERT, D_MODEL), D_EXPERT ** -0.5, 0.109375, ((0, 2), (2, 16)), (2, 1, 16, 2.0), jnp.float32)
    other_down = noise(streams_of[1], (EXPERTS, D_EXPERT, D_MODEL), (D_EXPERT * 4) ** -0.5, 0.0390625, ((0, 2), (2, 16)))
    router_weight = noise(streams_of[2], (D_MODEL, EXPERTS), D_MODEL ** -0.5, 0.09375, ((0, 16), (1, 2)), jnp.float32)
    router_gain = jnp.clip(1.0 + 0.15 * jax.random.normal(streams_of[3], (D_MODEL,), jnp.float32), 0.25, 1.75)
    return {"train_down": train_down, "other_down": other_down, "router_weight": router_weight, "router_gain": router_gain}


def reference(train_down, other_down, router_weight, router_gain):
    latest_down = train_down + other_down.astype(jnp.float32)
    scale_down = jnp.max(jnp.abs(latest_down), axis=2)
    ready_down = (latest_down / jnp.expand_dims(scale_down, 2)).astype(jnp.bfloat16)
    serve_router = (router_weight * router_gain[:, None]).astype(jnp.bfloat16)
    return ready_down, scale_down, serve_router
```

```python
import functools

import jax
import jax.numpy as jnp
from jax import lax
from jax.experimental import pallas as pl
from jax.experimental.pallas import tpu as pltpu
from jax.sharding import PartitionSpec as P

MESH = pl.DeviceIdType.MESH
LANES = 128


def partner_of(me, step, count):
    if count & (count - 1):
        return lax.rem(me + step, count)
    other, bit = me, 1
    while bit < count:
        if step & bit:
            other = other + bit * (1 - 2 * lax.rem(lax.div(me, bit), 2))
        bit *= 2
    return other


def origin_of(me, step, count):
    if count & (count - 1):
        return lax.rem(me + count - step, count)
    return partner_of(me, step, count)


def kernel(count, train, other, ready, scale, t_buf, o_buf, narrow, peak, peaks, scales,
           load_sem, peak_send, peak_recv, scale_send, scale_recv, data_send, data_recv, own_sem):
    experts, _, rows, columns = train.shape
    starts = [min(LANES * i, rows - LANES) for i in range(pl.cdiv(rows, LANES))]
    blocks = len(starts)
    me, bank = lax.axis_index("zero"), lax.axis_index("bank")
    steps = list(range(count - 1, 0, -1))

    def loads(index):
        slot, expert = lax.rem(index, 2), lax.rem(index, experts)
        return (pltpu.make_async_copy(train.at[expert], t_buf.at[slot], load_sem.at[0, slot]),
                pltpu.make_async_copy(other.at[expert], o_buf.at[slot], load_sem.at[1, slot]))

    def remote(source, target, sends, receives, step):
        return pltpu.make_async_remote_copy(
            src_ref=source, dst_ref=target, send_sem=sends, recv_sem=receives,
            device_id=(bank, partner_of(me, step, count)), device_id_type=MESH)

    def latest(slot, part, start):
        span = pl.ds(start, LANES)
        return t_buf[slot, part, span, :] + o_buf[slot, part, span, :].astype(jnp.float32)

    def advance(index):
        @pl.when(index + 1 < 2 * experts)
        def _():
            for copy in loads(index + 1):
                copy.start()
        for copy in loads(index):
            copy.wait()

    for copy in loads(jnp.int32(0)):
        copy.start()
    barrier = pltpu.get_barrier_semaphore()
    for step in steps:
        pl.semaphore_signal(barrier, inc=1, device_id=(bank, partner_of(me, step, count)), device_id_type=MESH)

    @pl.loop(0, experts)
    def _(expert):
        advance(expert)
        slot = lax.rem(expert, 2)

        @pl.loop(0, count)
        def _(part):
            for block, start in enumerate(starts):
                value = jnp.abs(latest(slot, part, start))
                folded = value[:, :LANES]
                for column in range(LANES, columns, LANES):
                    folded = jnp.maximum(folded, value[:, column:column + LANES])
                peak[part, pl.ds(expert * blocks + block, 1), :] = jnp.max(folded.T, axis=0, keepdims=True)

    pl.semaphore_wait(barrier, count - 1)
    for step in steps:
        remote(peak.at[partner_of(me, step, count)], peaks.at[me], peak_send, peak_recv, step).start()
    pltpu.make_async_copy(peaks.at[pl.ds(0, count - 1)], peaks.at[pl.ds(0, count - 1)], peak_recv).wait()
    total = peak[me]
    for step in steps:
        total = jnp.maximum(total, peaks[origin_of(me, step, count)])
    scales[me] = total
    scale[...] = total
    for step in steps:
        remote(scales.at[me], scales.at[me], scale_send, scale_recv, step).start()
    pltpu.make_async_copy(scales.at[pl.ds(0, count - 1)], scales.at[pl.ds(0, count - 1)], scale_recv).wait()

    mine = pl.ds(pl.multiple_of(me * columns, LANES), columns)

    @pl.loop(0, experts)
    def _(expert):
        advance(expert + experts)
        slot = lax.rem(expert + experts, 2)

        @pl.loop(0, count)
        def _(part):
            for block, start in enumerate(starts):
                factor = 1.0 / scales[part, pl.ds(expert * blocks + block, 1), :]
                factor = jnp.broadcast_to(factor, (LANES, LANES)).T
                value = latest(slot, part, start)
                for column in range(0, columns, LANES):
                    narrow[expert, part, pl.ds(start, LANES), pl.ds(column, LANES)] = (
                        value[:, column:column + LANES] * factor).astype(narrow.dtype)

        for step in steps:
            remote(narrow.at[expert, partner_of(me, step, count)], ready.at[expert, :, mine],
                   data_send, data_recv, step).start()
        pltpu.make_async_copy(narrow.at[expert, me], ready.at[expert, :, mine], own_sem).start()

    pltpu.make_async_copy(peak.at[pl.ds(0, count - 1)], peak.at[pl.ds(0, count - 1)], peak_send).wait()
    pltpu.make_async_copy(peak.at[pl.ds(0, count - 1)], peak.at[pl.ds(0, count - 1)], scale_send).wait()
    sent = narrow.at[:, pl.ds(0, count - 1)]
    pltpu.make_async_copy(sent, sent, data_send).wait()
    pltpu.make_async_copy(narrow.at[:, 0], narrow.at[:, 0], own_sem).wait()
    got = ready.at[:, :, pl.ds(0, (count - 1) * columns)]
    pltpu.make_async_copy(got, got, data_recv).wait()


def local(count, train_down, other_down, router_weight, router_gain):
    experts, length, columns = train_down.shape
    rows = length // count
    blocks = pl.cdiv(rows, LANES)
    split = (experts, count, rows, columns)
    anywhere = pl.BlockSpec(memory_space=pl.ANY)
    ready_down, scale = pl.pallas_call(
        functools.partial(kernel, count),
        out_shape=(jax.ShapeDtypeStruct((experts, rows, count * columns), jnp.bfloat16),
                   jax.ShapeDtypeStruct((experts * blocks, LANES), jnp.float32)),
        in_specs=[anywhere, anywhere],
        out_specs=(anywhere, pl.BlockSpec(memory_space=pltpu.VMEM)),
        scratch_shapes=[
            pltpu.VMEM((2,) + split[1:], jnp.float32),
            pltpu.VMEM((2,) + split[1:], jnp.bfloat16),
            pltpu.VMEM(split, jnp.bfloat16),
            pltpu.VMEM((count, experts * blocks, LANES), jnp.float32),
            pltpu.VMEM((count, experts * blocks, LANES), jnp.float32),
            pltpu.VMEM((count, experts * blocks, LANES), jnp.float32),
            pltpu.SemaphoreType.DMA((2, 2)),
        ] + [pltpu.SemaphoreType.DMA] * 7,
        compiler_params=pltpu.CompilerParams(
            collective_id=0, has_side_effects=True, vmem_limit_bytes=60 * 1024 * 1024),
    )(train_down.reshape(split), other_down.reshape(split))
    scale = scale.reshape(experts, blocks, LANES)
    pieces = [scale[:, block] for block in range(blocks - 1)]
    scale_down = jnp.concatenate(pieces + [scale[:, blocks - 1, LANES * blocks - rows:]], axis=1)
    part_router = (router_weight * router_gain[:, None]).astype(jnp.bfloat16)
    row_router = lax.all_gather(part_router, "zero", axis=0, tiled=True)
    serve_router = lax.all_gather(row_router, "bank", axis=1, tiled=True)
    return (ready_down, scale_down, serve_router)


def solution(mesh):
    in_specs = (P("bank", None, "zero"), P("bank", None, "zero"), P("zero", "bank"), P("zero"))
    out_specs = (P("bank", "zero", None), P("bank", "zero"), P())
    body = functools.partial(local, mesh.shape["zero"])
    return jax.shard_map(body, mesh=mesh, in_specs=in_specs, out_specs=out_specs, check_vma=False)
```

```python
import functools

import jax
import jax.numpy as jnp
from jax import lax
from jax.experimental import pallas as pl
from jax.experimental.pallas import tpu as pltpu
from jax.sharding import PartitionSpec as P

MESH = pl.DeviceIdType.MESH
LANES = 128


def partner_of(me, step, count):
    if count & (count - 1):
        return lax.rem(me + step, count)
    other, bit = me, 1
    while bit < count:
        if step & bit:
            other = other + bit * (1 - 2 * lax.rem(lax.div(me, bit), 2))
        bit *= 2
    return other


def origin_of(me, step, count):
    if count & (count - 1):
        return lax.rem(me + count - step, count)
    return partner_of(me, step, count)


def kernel(count, banks, train, other, weight, gain, ready, scale, router, t_buf, o_buf, narrow, pieces, gathered,
           peak_a, peaks_a, scales_a, peak_b, peaks_b, scales_b, load_sem, peak_send, peak_recv, scale_send, scale_recv,
           bank_send, bank_recv, router_send, router_recv, data_send, data_recv, own_sem):
    experts, _, rows, columns = train.shape
    starts = [min(LANES * i, rows - LANES) for i in range(pl.cdiv(rows, LANES))]
    blocks = len(starts)
    lead = lead_of(experts)
    me, bank = lax.axis_index("zero"), lax.axis_index("bank")
    steps = list(range(count - 1, 0, -1))
    groups = ((0, peak_a, peaks_a, scales_a), (lead, peak_b, peaks_b, scales_b))

    def loads(expert, slot):
        return (pltpu.make_async_copy(train.at[expert], t_buf.at[slot], load_sem.at[0, slot]),
                pltpu.make_async_copy(other.at[expert], o_buf.at[slot], load_sem.at[1, slot]))

    def remote(source, target, sends, receives, step):
        return pltpu.make_async_remote_copy(
            src_ref=source, dst_ref=target, send_sem=sends, recv_sem=receives,
            device_id=(bank, partner_of(me, step, count)), device_id_type=MESH)

    def settle(ref, semaphore):
        pltpu.make_async_copy(ref, ref, semaphore).wait()

    def latest(slot, part, start):
        span = pl.ds(start, LANES)
        return t_buf[slot, part, span, :] + o_buf[slot, part, span, :].astype(jnp.float32)

    def find_peaks(group, expert, slot):
        first, peak, _, _ = groups[group]

        @pl.loop(0, count)
        def _(part):
            for block, start in enumerate(starts):
                value = jnp.abs(latest(slot, part, start))
                folded = value[:, :LANES]
                for column in range(LANES, columns, LANES):
                    folded = jnp.maximum(folded, value[:, column:column + LANES])
                peak[part, pl.ds((expert - first) * blocks + block, 1), :] = jnp.max(folded.T, axis=0, keepdims=True)

    mine = pl.ds(pl.multiple_of(me * columns, LANES), columns)

    def normalise(group, expert, slot):
        first, _, _, scales = groups[group]

        @pl.loop(0, count)
        def _(part):
            for block, start in enumerate(starts):
                factor = 1.0 / scales[part, pl.ds((expert - first) * blocks + block, 1), :]
                factor = jnp.broadcast_to(factor, (LANES, LANES)).T
                value = latest(slot, part, start)
                for column in range(0, columns, LANES):
                    narrow[expert, part, pl.ds(start, LANES), pl.ds(column, LANES)] = (
                        value[:, column:column + LANES] * factor).astype(narrow.dtype)

        for step in steps:
            remote(narrow.at[expert, partner_of(me, step, count)], ready.at[expert, :, mine],
                   data_send, data_recv, step).start()
        pltpu.make_async_copy(narrow.at[expert, me], ready.at[expert, :, mine], own_sem).start()

    def send_peaks(group):
        _, peak, peaks, _ = groups[group]
        for step in steps:
            remote(peak.at[partner_of(me, step, count)], peaks.at[me],
                   peak_send.at[group], peak_recv.at[group], step).start()

    def send_scales(group):
        first, peak, peaks, scales = groups[group]
        settle(peaks.at[pl.ds(0, count - 1)], peak_recv.at[group])
        total = peak[me]
        for step in steps:
            total = jnp.maximum(total, peaks[origin_of(me, step, count)])
        scales[me] = total
        scale[pl.ds(first * blocks, total.shape[0]), :] = total
        for step in steps:
            remote(scales.at[me], scales.at[me], scale_send.at[group], scale_recv.at[group], step).start()

    def take_scales(group):
        scales = groups[group][3]
        settle(scales.at[pl.ds(0, count - 1)], scale_recv.at[group])

    def meet():
        pl.semaphore_wait(pltpu.get_barrier_semaphore(), count - 1 + banks - 1)
        for step in range(1, banks):
            pltpu.make_async_remote_copy(
                src_ref=pieces.at[bank], dst_ref=pieces.at[bank], send_sem=bank_send, recv_sem=bank_recv,
                device_id=(partner_of(bank, step, banks), me), device_id_type=MESH).start()
        send_peaks(0)

    def share_router():
        if banks > 1:
            settle(pieces.at[pl.ds(0, banks - 1)], bank_recv)
        gathered[me] = pieces[...]
        for step in steps:
            remote(pieces, gathered.at[me], router_send, router_recv, step).start()
        send_scales(0)

    near, far = min(lead + 1, experts), min(lead + 2, experts)
    rest = lead < experts
    plan = [
        (find_peaks, 0, 0, lead, meet),
        (find_peaks, 1, lead, near, share_router),
        (find_peaks, 1, near, far, lambda: take_scales(0)),
        (normalise, 0, 0, 1, None),
        (find_peaks, 1, far, experts, (lambda: send_peaks(1)) if rest else None),
        (normalise, 0, 1, min(2, lead), (lambda: send_scales(1)) if rest else None),
        (normalise, 0, min(2, lead), lead, (lambda: take_scales(1)) if rest else None),
        (normalise, 1, lead, experts, None),
    ]

    for copy in loads(0, 0):
        copy.start()
    barrier = pltpu.get_barrier_semaphore()
    for step in steps:
        pl.semaphore_signal(barrier, inc=1, device_id=(bank, partner_of(me, step, count)), device_id_type=MESH)
    for step in range(1, banks):
        pl.semaphore_signal(barrier, inc=1, device_id=(partner_of(bank, step, banks), me), device_id_type=MESH)
    pieces[bank] = (weight[...] * gain[...]).astype(pieces.dtype)

    place = 0
    for number, (work, group, first, last, then) in enumerate(plan):
        after = next((later[2] for later in plan[number + 1:] if later[2] < later[3]), None)

        def one(expert, position, coming):
            slot = lax.rem(position, 2)
            if coming is not None:
                for copy in loads(coming, 1 - slot):
                    copy.start()
            for copy in loads(expert, slot):
                copy.wait()
            work(group, expert, slot)

        if first < last:
            whole = last if after == last else last - 1
            if first < whole:
                @pl.loop(first, whole)
                def _(expert):
                    one(expert, expert - first + place, expert + 1)
            if whole < last:
                one(jnp.int32(whole), jnp.int32(whole - first + place), after)
            place += last - first
        if then is not None:
            then()

    for group in range(2 if rest else 1):
        peak = groups[group][1]
        settle(peak.at[pl.ds(0, count - 1)], peak_send.at[group])
        settle(peak.at[pl.ds(0, count - 1)], scale_send.at[group])
    if banks > 1:
        settle(pieces.at[pl.ds(0, banks - 1)], bank_send)
    settle(gathered.at[pl.ds(0, count - 1)], router_send)
    settle(gathered.at[pl.ds(0, count - 1)], router_recv)
    router[...] = gathered[...]
    settle(narrow.at[:, pl.ds(0, count - 1)], data_send)
    settle(narrow.at[:, 0], own_sem)
    settle(ready.at[:, :, pl.ds(0, (count - 1) * columns)], data_recv)


def lead_of(experts):
    return min(3, experts)


def local(count, banks, train_down, other_down, router_weight, router_gain):
    experts, length, columns = train_down.shape
    rows = length // count
    blocks = pl.cdiv(rows, LANES)
    split = (experts, count, rows, columns)
    share = (banks, router_weight.shape[1], router_weight.shape[0])
    lead = lead_of(experts)
    anywhere = pl.BlockSpec(memory_space=pl.ANY)
    inside = pl.BlockSpec(memory_space=pltpu.VMEM)
    tables = [pltpu.VMEM((count, blocks * size, LANES), jnp.float32)
              for size in (lead, max(experts - lead, 1)) for _ in range(3)]
    ready_down, scale, router = pl.pallas_call(
        functools.partial(kernel, count, banks),
        out_shape=(jax.ShapeDtypeStruct((experts, rows, count * columns), jnp.bfloat16),
                   jax.ShapeDtypeStruct((experts * blocks, LANES), jnp.float32),
                   jax.ShapeDtypeStruct((count,) + share, jnp.bfloat16)),
        in_specs=[anywhere, anywhere, inside, inside],
        out_specs=(anywhere, inside, inside),
        scratch_shapes=[
            pltpu.VMEM((2,) + split[1:], jnp.float32),
            pltpu.VMEM((2,) + split[1:], jnp.bfloat16),
            pltpu.VMEM(split, jnp.bfloat16),
            pltpu.VMEM(share, jnp.bfloat16),
            pltpu.VMEM((count,) + share, jnp.bfloat16),
        ] + tables + [pltpu.SemaphoreType.DMA((2, 2))] + [pltpu.SemaphoreType.DMA((2,))] * 4
        + [pltpu.SemaphoreType.DMA] * 7,
        compiler_params=pltpu.CompilerParams(
            collective_id=0, has_side_effects=True, vmem_limit_bytes=60 * 1024 * 1024),
    )(train_down.reshape(split), other_down.reshape(split), router_weight.T, router_gain[None, :])
    scale = scale.reshape(experts, blocks, LANES)
    parts = [scale[:, block] for block in range(blocks - 1)]
    scale_down = jnp.concatenate(parts + [scale[:, blocks - 1, LANES * blocks - rows:]], axis=1)
    serve_router = router.transpose(0, 3, 1, 2).reshape(count * share[2], banks * share[1])
    return (ready_down, scale_down, serve_router)


def solution(mesh):
    in_specs = (P("bank", None, "zero"), P("bank", None, "zero"), P("zero", "bank"), P("zero"))
    out_specs = (P("bank", "zero", None), P("bank", "zero"), P())
    body = functools.partial(local, mesh.shape["zero"], mesh.shape["bank"])
    return jax.shard_map(body, mesh=mesh, in_specs=in_specs, out_specs=out_specs, check_vma=False)
```
